32 devices in a mesh: grp: 2 (over x), seq: 16 (over z, y, core).
Axes of the slice: x: 2, y: 2, z: 4, core: 2. Of those that a mesh axis runs over, the one named last changes fastest.
Arguments:
- queries: bfloat16 [256, 4096], P(('grp', 'seq')), parts along dimension 0, may hold values from -9 to 9
- question_keys: bfloat16 [256, 2048], P(('grp', 'seq')), parts along dimension 0, may hold values from -4 to 4
- question_values: bfloat16 [256, 2048], P(('grp', 'seq')), parts along dimension 0, may hold values from -5 to 5
- doc_keys: bfloat16 [16384, 2048], P(('grp', 'seq')), parts along dimension 0, may hold values from -4 to 4
- doc_values: bfloat16 [16384, 2048], P(('grp', 'seq')), parts along dimension 0, may hold values from -5 to 5
- lengths: int32 [2], P('grp'), parts along dimension 0, may hold values from 4 to 128
- offsets: int32 [2], P('grp'), parts along dimension 0, may hold values from 2 to 8192, as said below
Outputs:
- attended: bfloat16 [256, 4096], P(('grp', 'seq')), parts along dimension 0
The draws below stay inside these ranges and needn't reach their ends.
There are 2 independent parts, one for each index of `grp`. The reference program is written for one: setup_inputs(seed, part) draws one part's arguments, and reference() takes and returns one part's arrays. A program takes and returns all parts, laid end to end along the dimension named above; each array names one. Nothing has to cross between parts.
Inputs may be any that keep to these rules, and one draw needn't show every extreme that they name: Some question has offsets equal to 8192.
All inputs are finite; a program needn't handle non-finite values.
Results may differ from the reference program's by a relative error of at most 0.0029.
Values may be sent and summed in bfloat16 or wider, within the bound.
No kernel may reach another device: no remote copies, remote signals or barrier semaphores. Data moves between devices by JAX's collectives and lax.ppermute only.
A program may use at most 64 MiB of HBM per device.

```python
import jax
import jax.numpy as jnp
from jax import lax

H = 32
KVH = 16
HD = 128
QSCALE = 144
QL = 128
NQ = 1
DOC_DEV = 512
QT = 128
DOC = 8192
N_SEQ = 16


def draw_queries(key, part):
    values = 3.0 * jax.random.normal(jax.random.fold_in(key, 11), (NQ * QL, H * HD), jnp.float32)
    values = jnp.clip(values, -9.0, 9.0)
    return values.astype(jnp.bfloat16)


def draw_doc_keys(key, part):
    values = jax.random.normal(jax.random.fold_in(key, 13), (DOC, KVH * HD), jnp.float32)
    values = jnp.clip(values, -4.0, 4.0)
    return values.astype(jnp.bfloat16)


def draw_offsets(key, part):
    spread = jax.random.randint(jax.random.fold_in(key, 3), (NQ,), 0, DOC - 1)
    shifts = jax.random.randint(jax.random.fold_in(key, 5), (NQ,), 0, 11)
    result = 2 + jnp.right_shift(spread, shifts)
    chosen = jax.random.randint(jax.random.fold_in(key, 9), (), 0, NQ)
    result = jnp.where(jnp.arange(NQ, dtype=jnp.int32) == chosen, DOC, result)
    return result.astype(jnp.int32)


def levels(rng, dims, split, least, top_value):
    def one(dim, parts):
        heights = jax.random.uniform(jax.random.fold_in(jax.random.fold_in(rng, 6), dim), (parts,), jnp.float32, least / len(split), top_value / len(split))
        return jnp.repeat(jnp.exp(heights), dims[dim] // parts).reshape((-1,) + (1,) * (len(dims) - dim - 1))

    loudness = one(*split[0])
    for cut in split[1:]:
        loudness = loudness * one(*cut)
    return loudness


def normal_values(key, dims, width, most, shards=(), held_as=jnp.bfloat16):
    values = width * jax.random.normal(key, dims, jnp.float32)
    if shards:
        values = values * levels(key, dims, shards, -0.22, 0.18)
    return jnp.clip(values, -most, most).astype(held_as)


def setup_inputs(seed: int = 0, part: int = 0) -> dict:
    keys = jax.random.split(jax.random.key(seed), 8)
    part_keys = jax.random.split(jax.random.fold_in(keys[7], part), 8)
    queries = draw_queries(jax.random.fold_in(jax.random.fold_in(keys[7], part), 71), part)
    question_keys = normal_values(part_keys[1], (QT, KVH * HD), 1.0, 4.0, ((0, 16),))
    question_values = normal_values(part_keys[2], (QT, KVH * HD), 1.0, 5.0, ((0, 16),))
    doc_keys = draw_doc_keys(jax.random.fold_in(jax.random.fold_in(keys[7], part), 71), part)
    doc_values = normal_values(part_keys[4], (DOC, KVH * HD), 1.0, 5.0, ((0, 16),))
    lengths = jax.random.randint(part_keys[5], (NQ,), 4, QL + 1).astype(jnp.int32)
    offsets = draw_offsets(jax.random.fold_in(jax.random.fold_in(keys[7], part), 71), part)
    return {"queries": queries, "question_keys": question_keys, "question_values": question_values, "doc_keys": doc_keys, "doc_values": doc_values, "lengths": lengths, "offsets": offsets}


MASKED = -1.0e30


def row_tables(start, count, lengths, offsets):
    rows = start + jnp.arange(count, dtype=jnp.int32)
    question = rows // QL
    position = rows % QL
    owner_table = question[:, None] == jnp.arange(NQ, dtype=jnp.int32)[None, :]
    row_length = jnp.sum(jnp.where(owner_table, lengths[None, :], 0), axis=1)
    row_offset = jnp.sum(jnp.where(owner_table, offsets[None, :], 0), axis=1)
    return question, position, position < row_length, row_offset


def rounded(values):
    narrow = lax.optimization_barrier(values.astype(jnp.bfloat16))
    return narrow.astype(jnp.float32)


def reference(queries, question_keys, question_values, doc_keys, doc_values, lengths, offsets):
    total_rows = NQ * QL
    rows_block = total_rows // N_SEQ
    per_group = H // KVH
    factor_q = QSCALE ** -0.5
    question, position, live_rows, row_offset = row_tables(0, total_rows, lengths, offsets)
    query_all = queries.astype(jnp.float32).reshape(total_rows, KVH, per_group, HD)

    def visit(state, block):
        row_top, numer, denom = state
        doc_start = (block * DOC_DEV).astype(jnp.int32)
        self_start = (block * rows_block).astype(jnp.int32)
        key_doc = lax.dynamic_slice_in_dim(doc_keys, doc_start, DOC_DEV, 0).astype(jnp.float32).reshape(DOC_DEV, KVH, HD)
        value_doc = lax.dynamic_slice_in_dim(doc_values, doc_start, DOC_DEV, 0).astype(jnp.float32).reshape(DOC_DEV, KVH, HD)
        key_self = lax.dynamic_slice_in_dim(question_keys, self_start, rows_block, 0).astype(jnp.float32).reshape(rows_block, KVH, HD)
        value_self = lax.dynamic_slice_in_dim(question_values, self_start, rows_block, 0).astype(jnp.float32).reshape(rows_block, KVH, HD)
        doc_places = doc_start + jnp.arange(DOC_DEV, dtype=jnp.int32)
        self_rows = self_start + jnp.arange(rows_block, dtype=jnp.int32)
        mask_doc = live_rows[:, None] & (doc_places[None, :] < row_offset[:, None])
        mask_self = live_rows[:, None] & (self_rows[None, :] // QL == question[:, None]) & (self_rows[None, :] % QL <= position[:, None])
        mask_doc = mask_doc[:, None, None, :]
        mask_self = mask_self[:, None, None, :]
        scores_doc = jnp.einsum("rgjd,kgd->rgjk", query_all, key_doc) * factor_q
        scores_self = jnp.einsum("rgjd,kgd->rgjk", query_all, key_self) * factor_q
        scores_doc = jnp.where(mask_doc, scores_doc, MASKED)
        scores_self = jnp.where(mask_self, scores_self, MASKED)
        block_top = jnp.maximum(jnp.max(scores_doc, axis=-1), jnp.max(scores_self, axis=-1))
        weights_doc = rounded(jnp.where(mask_doc, jnp.exp(scores_doc - block_top[..., None]), 0.0))
        weights_self = rounded(jnp.where(mask_self, jnp.exp(scores_self - block_top[..., None]), 0.0))
        block_num = jnp.einsum("rgjk,kgd->rgjd", weights_doc, value_doc) + jnp.einsum("rgjk,kgd->rgjd", weights_self, value_self)
        block_den = jnp.sum(weights_doc, axis=-1) + jnp.sum(weights_self, axis=-1)
        new_top = jnp.maximum(row_top, block_top)
        old_factor = jnp.exp(row_top - new_top)
        new_factor = jnp.exp(block_top - new_top)
        numer = numer * old_factor[..., None] + block_num * new_factor[..., None]
        denom = denom * old_factor + block_den * new_factor
        return (new_top, numer, denom), None

    start_state = (jnp.full((total_rows, KVH, per_group), MASKED, jnp.float32),
                   jnp.zeros((total_rows, KVH, per_group, HD), jnp.float32),
                   jnp.zeros((total_rows, KVH, per_group), jnp.float32))
    final_state, unused = lax.scan(visit, start_state, jnp.arange(N_SEQ, dtype=jnp.int32))
    row_top, numer, denom = final_state
    safe_den = jnp.where(live_rows[:, None, None], denom, 1.0)
    result = numer / safe_den[..., None]
    result = jnp.where(live_rows[:, None, None, None], result, 0.0)
    return result.reshape(total_rows, H * HD).astype(jnp.bfloat16)
```

```python
import functools
import math

import jax
import jax.numpy as jnp
from jax import lax
from jax.experimental import pallas as pl
from jax.experimental.pallas import tpu as pltpu
from jax.sharding import PartitionSpec as P

H = 32
KVH = 16
HD = 128
QSCALE = 144
QL = 128
NQ = 1


MASKED = -1e30
LANES = 128
SCALE2 = QSCALE ** (-0.5) * math.log2(math.e)


def split3(x):
    hi = x.astype(jnp.bfloat16).astype(jnp.float32)
    rest = x - hi
    mid = rest.astype(jnp.bfloat16).astype(jnp.float32)
    return hi, mid, rest - mid


def attend_kernel(chips, rows, sc_ref, *refs):
    q_refs = refs[:chips]
    own_k, own_v, own_sk, own_sv, par_k, par_v = refs[chips : chips + 6]
    o_ref, lse_ref = refs[chips + 6 : chips + 8]
    msg_refs = refs[chips + 8 :]
    docs = own_k.shape[0]
    per_group = H // KVH
    groups = par_k.shape[1] // HD
    heads = groups * per_group
    pair = 2 * rows
    count = chips * pair
    chip, core, offset = sc_ref[0], sc_ref[1], sc_ref[2]
    me, other = chip * 2 + core, chip * 2 + 1 - core

    lane = lax.broadcasted_iota(jnp.int32, (1, docs), 1)
    bias_own = jnp.where(me * docs + lane < offset, 0.0, MASKED)
    bias_par = jnp.where(other * docs + lane < offset, 0.0, MASKED)
    r = lax.broadcasted_iota(jnp.int32, (per_group * count, pair), 0) % count
    block_chip = chip ^ (r // pair)
    parity = (r % pair) // rows
    position = (block_chip * 2 + jnp.where(parity == 0, core, 1 - core)) * rows + r % rows
    col = lax.broadcasted_iota(jnp.int32, (per_group * count, pair), 1)
    key_row = jnp.where(col < rows, me, other) * rows + col % rows
    is_own = col < rows
    seen = key_row <= position
    seen_own, seen_par = seen & is_own, seen & ~is_own
    ones = jnp.ones((docs, HD), jnp.bfloat16)
    ones_self = jnp.ones((rows, HD), jnp.bfloat16)
    zeros_self = jnp.zeros((rows, 2 * HD), jnp.bfloat16)
    stat_lane = lax.broadcasted_iota(jnp.int32, (count, LANES), 1)
    stats = jnp.zeros((count, LANES), jnp.float32)
    exact = jnp.zeros((pair, LANES), jnp.float32)
    dot = functools.partial(lax.dot_general, preferred_element_type=jnp.float32)
    nt = (((1,), (1,)), ((), ()))
    nn = (((1,), (0,)), ((), ()))

    for g in range(groups):
        own_cols = pl.ds(pl.multiple_of((core * groups + g) * HD, HD), HD)
        par_cols = slice(g * HD, (g + 1) * HD)
        q = jnp.concatenate(
            [
                ref[:, (g * per_group + j) * HD : (g * per_group + j + 1) * HD]
                for j in range(per_group)
                for ref in q_refs
            ],
            axis=0,
        )
        ks = jnp.concatenate([own_sk[:, own_cols], par_k[docs:, par_cols]], axis=0)
        s_own = dot(q, own_k[:, own_cols], nt) + bias_own
        s_par = dot(q, par_k[:docs, par_cols], nt) + bias_par
        s_self = dot(q, ks, nt)
        m_own = jnp.maximum(
            jnp.max(s_own, axis=1, keepdims=True),
            jnp.max(jnp.where(seen_own, s_self, MASKED), axis=1, keepdims=True),
        )
        m_par = jnp.maximum(
            jnp.max(s_par, axis=1, keepdims=True),
            jnp.max(jnp.where(seen_par, s_self, MASKED), axis=1, keepdims=True),
        )
        c_own, c_par = m_own * SCALE2, m_par * SCALE2
        w_own = jnp.exp2(s_own * SCALE2 - c_own).astype(jnp.bfloat16)
        w_par = jnp.exp2(s_par * SCALE2 - c_par).astype(jnp.bfloat16)
        w_self = jnp.where(
            seen, jnp.exp2(s_self * SCALE2 - jnp.where(is_own, c_own, c_par)), 0.0
        ).astype(jnp.bfloat16)
        v_self = jnp.concatenate(
            [
                jnp.concatenate([own_sv[:, own_cols], ones_self, zeros_self], axis=1),
                jnp.concatenate([zeros_self, par_v[docs:, par_cols], ones_self], axis=1),
            ],
            axis=0,
        )
        n_self = dot(w_self, v_self, nn)
        n_own = dot(w_own, jnp.concatenate([own_v[:, own_cols], ones], axis=1), nn)
        n_par = dot(w_par, jnp.concatenate([par_v[:docs, par_cols], ones], axis=1), nn)
        n_own = n_own + n_self[:, : 2 * HD]
        n_par = n_par + n_self[:, 2 * HD :]
        c_top = jnp.maximum(c_own, c_par)
        a, b = jnp.exp2(c_own - c_top), jnp.exp2(c_par - c_top)
        num = n_own[:, :HD] * a + n_par[:, :HD] * b
        den = n_own[:, HD:] * a + n_par[:, HD:] * b
        out = num / den
        lse = c_top + jnp.log2(den)
        hi, mid, lo = split3(lse)
        for j in range(per_group):
            h = g * per_group + j
            part = slice(j * count, (j + 1) * count)
            val = jnp.where(
                stat_lane < heads,
                hi[part],
                jnp.where(stat_lane < 2 * heads, mid[part], lo[part]),
            )
            stats = jnp.where(stat_lane % heads == h, val, stats)
            exact = jnp.where(stat_lane[:pair] == h, lse[j * count : j * count + pair], exact)
            cols = slice(h * HD, (h + 1) * HD)
            o_ref[:, cols] = out[j * count : j * count + pair]
            for k in range(1, chips):
                at = j * count + k * pair
                msg_refs[k - 1][:, cols] = out[at : at + pair].astype(jnp.bfloat16)
    lse_ref[...] = exact
    for k in range(1, chips):
        msg_refs[k - 1][:, heads * HD :] = stats[k * pair : (k + 1) * pair].astype(jnp.bfloat16)


def combine_kernel(chips, rows, sc_ref, o_ref, lse_ref, *refs):
    msg_refs = refs[: chips - 1]
    mine_ref, theirs_ref = refs[chips - 1 :]
    heads = o_ref.shape[1] // HD
    pair = 2 * rows
    chip, core, length = sc_ref[0], sc_ref[1], sc_ref[3]
    lses = [lse_ref[...]]
    for ref in msg_refs:
        s = ref[:, heads * HD :].astype(jnp.float32)
        lses.append(
            s + pltpu.roll(s, LANES - heads, 1) + pltpu.roll(s, LANES - 2 * heads, 1)
        )
    top = functools.reduce(jnp.maximum, lses)
    scales = [jnp.exp2(x - top) for x in lses]
    total = functools.reduce(jnp.add, scales)
    i = lax.broadcasted_iota(jnp.int32, (pair, 1), 0)
    position = (chip * 2 + jnp.where(i < rows, core, 1 - core)) * rows + i % rows
    live = position < length
    scales = [jnp.where(live, x / total, 0.0) for x in scales]
    for h in range(heads):
        cols = slice(h * HD, (h + 1) * HD)
        acc = o_ref[:, cols] * scales[0][:, h : h + 1]
        for ref, x in zip(msg_refs, scales[1:]):
            acc = acc + ref[:, cols].astype(jnp.float32) * x[:, h : h + 1]
        acc = acc.astype(jnp.bfloat16)
        mine_ref[:, cols] = acc[:rows]
        theirs_ref[:, cols] = acc[rows:]


def by_permutes(queries, question_keys, question_values, doc_keys, doc_values, lengths, offsets):
    rows = queries.shape[0]
    docs = doc_keys.shape[0]
    size = lax.axis_size("seq")
    chips = size // 2
    index = lax.axis_index("seq")
    chip, core = index // 2, index % 2
    q_half, kv_half = H * HD // 2, KVH * HD // 2
    heads = H // 2
    pair = 2 * rows

    def swap(x, flip):
        return lax.ppermute(x, "seq", [(i, i ^ flip) for i in range(size)])

    def half(x, which, width):
        return lax.dynamic_slice_in_dim(x, which * width, width, axis=1)

    got = swap(half(queries, 1 - core, q_half), 1)
    block = jnp.concatenate([half(queries, core, q_half), got], axis=0)
    blocks = {0: block}
    top = chips // 2
    if top:
        blocks[top] = swap(block, 2 * top)
    for k in range(1, top):
        blocks[k] = swap(block, 2 * k)
    for k in range(1, top):
        blocks[top ^ k] = swap(blocks[top], 2 * k)
    par_k = swap(jnp.concatenate([half(doc_keys, 1 - core, kv_half), half(question_keys, 1 - core, kv_half)], axis=0), 1)
    par_v = swap(jnp.concatenate([half(doc_values, 1 - core, kv_half), half(question_values, 1 - core, kv_half)], axis=0), 1)
    scalars = jnp.stack([chip, core, offsets[0], lengths[0]]).astype(jnp.int32)
    smem = pl.BlockSpec(memory_space=pltpu.SMEM)
    vmem = pl.BlockSpec(memory_space=pltpu.VMEM)
    width = heads * HD + LANES
    outs = pl.pallas_call(
        functools.partial(attend_kernel, chips, rows),
        out_shape=[
            jax.ShapeDtypeStruct((pair, heads * HD), jnp.float32),
            jax.ShapeDtypeStruct((pair, LANES), jnp.float32),
        ]
        + [jax.ShapeDtypeStruct((pair, width), jnp.bfloat16)] * (chips - 1),
        in_specs=[smem] + [vmem] * (chips + 6),
        out_specs=[vmem] * (chips + 1),
        name="attend",
    )(
        scalars,
        *[blocks[k] for k in range(chips)],
        doc_keys,
        doc_values,
        question_keys,
        question_values,
        par_k,
        par_v,
    )
    own, own_lse, sent = outs[0], outs[1], outs[2:]
    order = sorted(range(1, chips), key=lambda k: -k)
    came = {k: swap(sent[k - 1], 2 * k) for k in order}
    mine, theirs = pl.pallas_call(
        functools.partial(combine_kernel, chips, rows),
        out_shape=[jax.ShapeDtypeStruct((rows, heads * HD), jnp.bfloat16)] * 2,
        in_specs=[smem] + [vmem] * (chips + 1),
        out_specs=[vmem] * 2,
        name="combine",
    )(scalars, own, own_lse, *[came[k] for k in range(1, chips)])
    got = swap(theirs, 1)
    return jnp.where(
        core == 0,
        jnp.concatenate([mine, got], axis=1),
        jnp.concatenate([got, mine], axis=1),
    )


def row_tables(start, count, lengths, offsets):
    rows = start + jnp.arange(count, dtype=jnp.int32)
    question = rows // QL
    position = rows % QL
    owner_table = question[:, None] == jnp.arange(NQ, dtype=jnp.int32)[None, :]
    row_length = jnp.sum(jnp.where(owner_table, lengths[None, :], 0), axis=1)
    row_offset = jnp.sum(jnp.where(owner_table, offsets[None, :], 0), axis=1)
    return (question, position, position < row_length, row_offset)


def by_collectives(queries, question_keys, question_values, doc_keys, doc_values, lengths, offsets):
    rows_local = queries.shape[0]
    doc_local = doc_keys.shape[0]
    device_count = lax.axis_size("seq")
    device_index = lax.axis_index("seq")
    total_rows = rows_local * device_count
    per_group = H // KVH
    factor_q = QSCALE ** (-0.5)
    key_doc = doc_keys.reshape(doc_local, KVH, HD)
    value_doc = doc_values.reshape(doc_local, KVH, HD)
    key_self = question_keys.reshape(rows_local, KVH, HD)
    value_self = question_values.reshape(rows_local, KVH, HD)
    doc_places = device_index * doc_local + jnp.arange(doc_local, dtype=jnp.int32)
    self_rows = device_index * rows_local + jnp.arange(rows_local, dtype=jnp.int32)
    whole = lax.all_gather(queries, "seq", axis=0, tiled=True)
    block_rows = math.gcd(total_rows, 512)
    block_count = total_rows // block_rows

    def one_block(start):
        piece = whole.reshape(block_rows, KVH, per_group, HD)
        question, position, live_rows, row_offset = row_tables(start, block_rows, lengths, offsets)
        mask_doc = live_rows[:, None] & (doc_places[None, :] < row_offset[:, None])
        mask_self = (
            live_rows[:, None]
            & (self_rows[None, :] // QL == question[:, None])
            & (self_rows[None, :] % QL <= position[:, None])
        )
        mask_doc = mask_doc[:, None, None, :]
        mask_self = mask_self[:, None, None, :]
        scores_doc = (
            jnp.einsum("rgjd,kgd->rgjk", piece, key_doc, preferred_element_type=jnp.float32)
            * factor_q
        )
        scores_self = (
            jnp.einsum("rgjd,kgd->rgjk", piece, key_self, preferred_element_type=jnp.float32)
            * factor_q
        )
        scores_doc = jnp.where(mask_doc, scores_doc, MASKED)
        scores_self = jnp.where(mask_self, scores_self, MASKED)
        block_top = jnp.maximum(jnp.max(scores_doc, axis=-1), jnp.max(scores_self, axis=-1))
        weights_doc = jnp.where(mask_doc, jnp.exp(scores_doc - block_top[..., None]), 0.0).astype(
            jnp.bfloat16
        )
        weights_self = jnp.where(
            mask_self, jnp.exp(scores_self - block_top[..., None]), 0.0
        ).astype(jnp.bfloat16)
        block_den = jnp.sum(weights_doc.astype(jnp.float32), axis=-1) + jnp.sum(
            weights_self.astype(jnp.float32), axis=-1
        )
        block_num = jnp.einsum(
            "rgjk,kgd->rgjd", weights_doc, value_doc, preferred_element_type=jnp.float32
        )
        block_num = block_num + jnp.einsum(
            "rgjk,kgd->rgjd", weights_self, value_self, preferred_element_type=jnp.float32
        )
        return (
            block_num.reshape(block_rows, H * HD),
            block_top.reshape(block_rows, H),
            block_den.reshape(block_rows, H),
        )

    starts = jnp.arange(block_count, dtype=jnp.int32) * block_rows
    numer, row_top, denom = lax.map(one_block, starts)
    numer = numer.reshape(total_rows, H * HD)
    row_top = row_top.reshape(total_rows, H)
    denom = denom.reshape(total_rows, H)
    got_num, got_top, got_den = (
        lax.all_to_all(numer[None], "seq", split_axis=1, concat_axis=0, tiled=True),
        lax.all_to_all(row_top[None], "seq", split_axis=1, concat_axis=0, tiled=True),
        lax.all_to_all(denom[None], "seq", split_axis=1, concat_axis=0, tiled=True),
    )
    overall = jnp.max(got_top, axis=0)
    rescale = jnp.exp(got_top - overall[None])
    total_num = jnp.sum(
        got_num.reshape(device_count, rows_local, H, HD) * rescale[:, :, :, None], axis=0
    )
    total_den = jnp.sum(got_den * rescale, axis=0)
    question, position, live_rows, row_offset = row_tables(
        device_index * rows_local, rows_local, lengths, offsets
    )
    safe_den = jnp.where(live_rows[:, None], total_den, 1.0)
    result = (total_num / safe_den[:, :, None]).reshape(rows_local, H * HD)
    return jnp.where(live_rows[:, None], result, 0.0).astype(jnp.bfloat16)


def solution(mesh):
    placed = (
        P(("grp", "seq"), None),
        P(("grp", "seq"), None),
        P(("grp", "seq"), None),
        P(("grp", "seq"), None),
        P(("grp", "seq"), None),
        P("grp"),
        P("grp"),
    )
    size = mesh.shape["seq"]
    few = size % 2 == 0 and size <= 16 and size & (size - 1) == 0
    return jax.shard_map(
        by_permutes if few else by_collectives,
        mesh=mesh,
        in_specs=placed,
        out_specs=P(("grp", "seq"), None),
        check_vma=False,
    )
```

```python
import functools
import math

import jax
import jax.numpy as jnp
from jax import lax
from jax.experimental import pallas as pl
from jax.experimental.pallas import tpu as pltpu
from jax.sharding import PartitionSpec as P

H = 32
KVH = 16
HD = 128
QSCALE = 144
QL = 128
NQ = 1


MASKED = -1e30
LANES = 128
SCALE2 = QSCALE ** (-0.5) * math.log2(math.e)

VMEM_GRANT = 24 << 20


def split3(x):
    hi = x.astype(jnp.bfloat16).astype(jnp.float32)
    rest = x - hi
    mid = rest.astype(jnp.bfloat16).astype(jnp.float32)
    return hi, mid, rest - mid


def attend_kernel(chips, rows, offset_ref, *refs):
    q_refs = refs[:chips]
    own_k, own_v, own_sk, own_sv, par_k, par_v = refs[chips : chips + 6]
    o_ref, lse_ref = refs[chips + 6 : chips + 8]
    msg_refs = refs[chips + 8 :]
    docs = own_k.shape[0]
    per_group = H // KVH
    groups = par_k.shape[1] // HD
    heads = groups * per_group
    pair = 2 * rows
    count = chips * pair
    index = lax.axis_index("seq")
    chip, core, offset = index // 2, index % 2, offset_ref[0]
    me, other = chip * 2 + core, chip * 2 + 1 - core

    lane = lax.broadcasted_iota(jnp.int32, (1, docs), 1)
    bias_own = jnp.where(me * docs + lane < offset, 0.0, MASKED)
    bias_par = jnp.where(other * docs + lane < offset, 0.0, MASKED)
    r = lax.broadcasted_iota(jnp.int32, (per_group * count, pair), 0) % count
    block_chip = chip ^ (r // pair)
    parity = (r % pair) // rows
    position = (block_chip * 2 + jnp.where(parity == 0, core, 1 - core)) * rows + r % rows
    col = lax.broadcasted_iota(jnp.int32, (per_group * count, pair), 1)
    key_row = jnp.where(col < rows, me, other) * rows + col % rows
    is_own = col < rows
    seen = key_row <= position
    seen_own, seen_par = seen & is_own, seen & ~is_own
    ones = jnp.ones((docs, HD), jnp.bfloat16)
    ones_self = jnp.ones((rows, HD), jnp.bfloat16)
    zeros_self = jnp.zeros((rows, 2 * HD), jnp.bfloat16)
    stat_lane = lax.broadcasted_iota(jnp.int32, (count, LANES), 1)
    stats = jnp.zeros((count, LANES), jnp.float32)
    exact = jnp.zeros((pair, LANES), jnp.float32)
    dot = functools.partial(lax.dot_general, preferred_element_type=jnp.float32)
    nt = (((1,), (1,)), ((), ()))
    nn = (((1,), (0,)), ((), ()))

    for g in range(groups):
        own_cols = pl.ds(pl.multiple_of((core * groups + g) * HD, HD), HD)
        par_cols = slice(g * HD, (g + 1) * HD)
        q = jnp.concatenate(
            [
                ref[:, (g * per_group + j) * HD : (g * per_group + j + 1) * HD]
                for j in range(per_group)
                for ref in q_refs
            ],
            axis=0,
        )
        ks = jnp.concatenate([own_sk[:, own_cols], par_k[docs:, par_cols]], axis=0)
        s_own = dot(q, own_k[:, own_cols], nt) + bias_own
        s_par = dot(q, par_k[:docs, par_cols], nt) + bias_par
        s_self = dot(q, ks, nt)
        m_own = jnp.maximum(
            jnp.max(s_own, axis=1, keepdims=True),
            jnp.max(jnp.where(seen_own, s_self, MASKED), axis=1, keepdims=True),
        )
        m_par = jnp.maximum(
            jnp.max(s_par, axis=1, keepdims=True),
            jnp.max(jnp.where(seen_par, s_self, MASKED), axis=1, keepdims=True),
        )
        c_own, c_par = m_own * SCALE2, m_par * SCALE2
        w_own = jnp.exp2(s_own * SCALE2 - c_own).astype(jnp.bfloat16)
        w_par = jnp.exp2(s_par * SCALE2 - c_par).astype(jnp.bfloat16)
        w_self = jnp.where(
            seen, jnp.exp2(s_self * SCALE2 - jnp.where(is_own, c_own, c_par)), 0.0
        ).astype(jnp.bfloat16)
        v_self = jnp.concatenate(
            [
                jnp.concatenate([own_sv[:, own_cols], ones_self, zeros_self], axis=1),
                jnp.concatenate([zeros_self, par_v[docs:, par_cols], ones_self], axis=1),
            ],
            axis=0,
        )
        n_self = dot(w_self, v_self, nn)
        n_own = dot(w_own, jnp.concatenate([own_v[:, own_cols], ones], axis=1), nn)
        n_par = dot(w_par, jnp.concatenate([par_v[:docs, par_cols], ones], axis=1), nn)
        n_own = n_own + n_self[:, : 2 * HD]
        n_par = n_par + n_self[:, 2 * HD :]
        c_top = jnp.maximum(c_own, c_par)
        a, b = jnp.exp2(c_own - c_top), jnp.exp2(c_par - c_top)
        num = n_own[:, :HD] * a + n_par[:, :HD] * b
        den = n_own[:, HD:] * a + n_par[:, HD:] * b
        out = num / den
        lse = c_top + jnp.log2(den)
        hi, mid, lo = split3(lse)
        for j in range(per_group):
            h = g * per_group + j
            part = slice(j * count, (j + 1) * count)
            val = jnp.where(
                stat_lane < heads,
                hi[part],
                jnp.where(stat_lane < 2 * heads, mid[part], lo[part]),
            )
            stats = jnp.where(stat_lane % heads == h, val, stats)
            exact = jnp.where(stat_lane[:pair] == h, lse[j * count : j * count + pair], exact)
            cols = slice(h * HD, (h + 1) * HD)
            o_ref[:, cols] = out[j * count : j * count + pair]
            for k in range(1, chips):
                at = j * count + k * pair
                msg_refs[k - 1][:, cols] = out[at : at + pair].astype(jnp.bfloat16)
    lse_ref[...] = exact
    for k in range(1, chips):
        msg_refs[k - 1][:, heads * HD :] = stats[k * pair : (k + 1) * pair].astype(jnp.bfloat16)


def combine_kernel(chips, rows, length_ref, o_ref, lse_ref, *refs):
    msg_refs = refs[: chips - 1]
    mine_ref, theirs_ref = refs[chips - 1 :]
    heads = o_ref.shape[1] // HD
    pair = 2 * rows
    index = lax.axis_index("seq")
    chip, core, length = index // 2, index % 2, length_ref[0]
    lses = [lse_ref[...]]
    for ref in msg_refs:
        s = ref[:, heads * HD :].astype(jnp.float32)
        lses.append(
            s + pltpu.roll(s, LANES - heads, 1) + pltpu.roll(s, LANES - 2 * heads, 1)
        )
    top = functools.reduce(jnp.maximum, lses)
    scales = [jnp.exp2(x - top) for x in lses]
    total = functools.reduce(jnp.add, scales)
    i = lax.broadcasted_iota(jnp.int32, (pair, 1), 0)
    position = (chip * 2 + jnp.where(i < rows, core, 1 - core)) * rows + i % rows
    live = position < length
    scales = [jnp.where(live, x / total, 0.0) for x in scales]
    for h in range(heads):
        cols = slice(h * HD, (h + 1) * HD)
        acc = o_ref[:, cols] * scales[0][:, h : h + 1]
        for ref, x in zip(msg_refs, scales[1:]):
            acc = acc + ref[:, cols].astype(jnp.float32) * x[:, h : h + 1]
        acc = acc.astype(jnp.bfloat16)
        mine_ref[:, cols] = acc[:rows]
        theirs_ref[:, cols] = acc[rows:]


def by_permutes(queries, question_keys, question_values, doc_keys, doc_values, lengths, offsets):
    rows = queries.shape[0]
    docs = doc_keys.shape[0]
    size = lax.axis_size("seq")
    chips = size // 2
    index = lax.axis_index("seq")
    chip, core = index // 2, index % 2
    q_half, kv_half = H * HD // 2, KVH * HD // 2
    heads = H // 2
    pair = 2 * rows

    def swap(x, flip):
        return lax.ppermute(x, "seq", [(i, i ^ flip) for i in range(size)])

    def half(x, which, width):
        return lax.dynamic_slice_in_dim(x, which * width, width, axis=1)

    got = swap(half(queries, 1 - core, q_half), 1)
    block = jnp.concatenate([half(queries, core, q_half), got], axis=0)
    blocks = {0: block}
    top = chips // 2
    if top:
        blocks[top] = swap(block, 2 * top)
    for k in range(1, top):
        blocks[k] = swap(block, 2 * k)
    for k in range(1, top):
        blocks[top ^ k] = swap(blocks[top], 2 * k)
    doc_keys, doc_values, question_keys, question_values, got = lax.optimization_barrier(
        (doc_keys, doc_values, question_keys, question_values, got)
    )
    par_k = swap(jnp.concatenate([half(doc_keys, 1 - core, kv_half), half(question_keys, 1 - core, kv_half)], axis=0), 1)
    par_v = swap(jnp.concatenate([half(doc_values, 1 - core, kv_half), half(question_values, 1 - core, kv_half)], axis=0), 1)
    smem = pl.BlockSpec(memory_space=pltpu.SMEM)
    vmem = pl.BlockSpec(memory_space=pltpu.VMEM)
    width = heads * HD + LANES
    outs = pl.pallas_call(
        functools.partial(attend_kernel, chips, rows),
        out_shape=[
            jax.ShapeDtypeStruct((pair, heads * HD), jnp.float32),
            jax.ShapeDtypeStruct((pair, LANES), jnp.float32),
        ]
        + [jax.ShapeDtypeStruct((pair, width), jnp.bfloat16)] * (chips - 1),
        in_specs=[smem] + [vmem] * (chips + 6),
        out_specs=[vmem] * (chips + 1),
        compiler_params=pltpu.CompilerParams(vmem_limit_bytes=VMEM_GRANT),
        name="attend",
    )(
        offsets,
        *[blocks[k] for k in range(chips)],
        doc_keys,
        doc_values,
        question_keys,
        question_values,
        par_k,
        par_v,
    )
    own, own_lse, sent = outs[0], outs[1], outs[2:]
    order = sorted(range(1, chips), key=lambda k: -k)
    came = {k: swap(sent[k - 1], 2 * k) for k in order}
    mine, theirs = pl.pallas_call(
        functools.partial(combine_kernel, chips, rows),
        out_shape=[jax.ShapeDtypeStruct((rows, heads * HD), jnp.bfloat16)] * 2,
        in_specs=[smem] + [vmem] * (chips + 1),
        out_specs=[vmem] * 2,
        compiler_params=pltpu.CompilerParams(vmem_limit_bytes=VMEM_GRANT),
        name="combine",
    )(lengths, own, own_lse, *[came[k] for k in range(1, chips)])
    got = swap(theirs, 1)
    return jnp.where(
        core == 0,
        jnp.concatenate([mine, got], axis=1),
        jnp.concatenate([got, mine], axis=1),
    )


def row_tables(start, count, lengths, offsets):
    rows = start + jnp.arange(count, dtype=jnp.int32)
    question = rows // QL
    position = rows % QL
    owner_table = question[:, None] == jnp.arange(NQ, dtype=jnp.int32)[None, :]
    row_length = jnp.sum(jnp.where(owner_table, lengths[None, :], 0), axis=1)
    row_offset = jnp.sum(jnp.where(owner_table, offsets[None, :], 0), axis=1)
    return (question, position, position < row_length, row_offset)


def by_collectives(queries, question_keys, question_values, doc_keys, doc_values, lengths, offsets):
    rows_local = queries.shape[0]
    doc_local = doc_keys.shape[0]
    device_count = lax.axis_size("seq")
    device_index = lax.axis_index("seq")
    total_rows = rows_local * device_count
    per_group = H // KVH
    factor_q = QSCALE ** (-0.5)
    key_doc = doc_keys.reshape(doc_local, KVH, HD)
    value_doc = doc_values.reshape(doc_local, KVH, HD)
    key_self = question_keys.reshape(rows_local, KVH, HD)
    value_self = question_values.reshape(rows_local, KVH, HD)
    doc_places = device_index * doc_local + jnp.arange(doc_local, dtype=jnp.int32)
    self_rows = device_index * rows_local + jnp.arange(rows_local, dtype=jnp.int32)
    whole = lax.all_gather(queries, "seq", axis=0, tiled=True)
    block_rows = math.gcd(total_rows, 512)
    block_count = total_rows // block_rows

    def one_block(start):
        piece = whole.reshape(block_rows, KVH, per_group, HD)
        question, position, live_rows, row_offset = row_tables(start, block_rows, lengths, offsets)
        mask_doc = live_rows[:, None] & (doc_places[None, :] < row_offset[:, None])
        mask_self = (
            live_rows[:, None]
            & (self_rows[None, :] // QL == question[:, None])
            & (self_rows[None, :] % QL <= position[:, None])
        )
        mask_doc = mask_doc[:, None, None, :]
        mask_self = mask_self[:, None, None, :]
        scores_doc = (
            jnp.einsum("rgjd,kgd->rgjk", piece, key_doc, preferred_element_type=jnp.float32)
            * factor_q
        )
        scores_self = (
            jnp.einsum("rgjd,kgd->rgjk", piece, key_self, preferred_element_type=jnp.float32)
            * factor_q
        )
        scores_doc = jnp.where(mask_doc, scores_doc, MASKED)
        scores_self = jnp.where(mask_self, scores_self, MASKED)
        block_top = jnp.maximum(jnp.max(scores_doc, axis=-1), jnp.max(scores_self, axis=-1))
        weights_doc = jnp.where(mask_doc, jnp.exp(scores_doc - block_top[..., None]), 0.0).astype(
            jnp.bfloat16
        )
        weights_self = jnp.where(
            mask_self, jnp.exp(scores_self - block_top[..., None]), 0.0
        ).astype(jnp.bfloat16)
        block_den = jnp.sum(weights_doc.astype(jnp.float32), axis=-1) + jnp.sum(
            weights_self.astype(jnp.float32), axis=-1
        )
        block_num = jnp.einsum(
            "rgjk,kgd->rgjd", weights_doc, value_doc, preferred_element_type=jnp.float32
        )
        block_num = block_num + jnp.einsum(
            "rgjk,kgd->rgjd", weights_self, value_self, preferred_element_type=jnp.float32
        )
        return (
            block_num.reshape(block_rows, H * HD),
            block_top.reshape(block_rows, H),
            block_den.reshape(block_rows, H),
        )

    starts = jnp.arange(block_count, dtype=jnp.int32) * block_rows
    numer, row_top, denom = lax.map(one_block, starts)
    numer = numer.reshape(total_rows, H * HD)
    row_top = row_top.reshape(total_rows, H)
    denom = denom.reshape(total_rows, H)
    got_num, got_top, got_den = (
        lax.all_to_all(numer[None], "seq", split_axis=1, concat_axis=0, tiled=True),
        lax.all_to_all(row_top[None], "seq", split_axis=1, concat_axis=0, tiled=True),
        lax.all_to_all(denom[None], "seq", split_axis=1, concat_axis=0, tiled=True),
    )
    overall = jnp.max(got_top, axis=0)
    rescale = jnp.exp(got_top - overall[None])
    total_num = jnp.sum(
        got_num.reshape(device_count, rows_local, H, HD) * rescale[:, :, :, None], axis=0
    )
    total_den = jnp.sum(got_den * rescale, axis=0)
    question, position, live_rows, row_offset = row_tables(
        device_index * rows_local, rows_local, lengths, offsets
    )
    safe_den = jnp.where(live_rows[:, None], total_den, 1.0)
    result = (total_num / safe_den[:, :, None]).reshape(rows_local, H * HD)
    return jnp.where(live_rows[:, None], result, 0.0).astype(jnp.bfloat16)


def solution(mesh):
    placed = (
        P(("grp", "seq"), None),
        P(("grp", "seq"), None),
        P(("grp", "seq"), None),
        P(("grp", "seq"), None),
        P(("grp", "seq"), None),
        P("grp"),
        P("grp"),
    )
    size = mesh.shape["seq"]
    few = size % 2 == 0 and size <= 16 and size & (size - 1) == 0
    return jax.shard_map(
        by_permutes if few else by_collectives,
        mesh=mesh,
        in_specs=placed,
        out_specs=P(("grp", "seq"), None),
        check_vma=False,
    )
```
